128 devices in a mesh: data: 1, sp: 128 (over z, y, x, core).
Axes of the slice: x: 4, y: 4, z: 4, core: 2. Of those that a mesh axis runs over, the one named last changes fastest.
Arguments:
- latents: bfloat16 [1, 256, 256, 384], P('data', 'sp')
- norms: float32 [4, 4, 384], replicated
- w_qkv: bfloat16 [4, 384, 3, 6, 64], replicated
- w_out: bfloat16 [4, 6, 64, 384], replicated
- w_up: bfloat16 [4, 384, 1536], replicated
- w_down: bfloat16 [4, 1536, 384], replicated
Outputs:
- output: bfloat16 [1, 256, 256, 384], P('data', None, 'sp')
All inputs are finite; a program needn't handle non-finite values.
Results may differ from the reference program's by a relative error of at most 0.015725.
Values are sent between devices in bfloat16 or wider.
A program may use at most 1 GiB of HBM per device.

```python
import math
import jax
import jax.numpy as jnp
from jax import lax

BATCH = 1
FRAMES = 256
PATCHES = 256
WIDTH = 384
HEADS = 6
BLOCKS = 4
HEAD_DIM = WIDTH // HEADS
HIDDEN = 4 * WIDTH
EPS = 1e-6
SPATIAL = (2, 'btqhe,btkhe->bthqk', 'bthqk,btkhe->btqhe')
TEMPORAL = (1, 'bqshe,bkshe->bshqk', 'bshqk,bkshe->bqshe')


def setup_inputs(seed: int = 0, part: int = 0) -> dict:
    base_key = jax.random.key(seed)
    part_key = jax.random.fold_in(base_key, part)
    time_key, space_key, noise_key = jax.random.split(part_key, 3)
    time_walk = jnp.cumsum(jax.random.normal(time_key, (BATCH, FRAMES, WIDTH), jnp.float32), axis=1) * (1.5 / math.sqrt(FRAMES))
    space_walk = jnp.cumsum(jax.random.normal(space_key, (BATCH, PATCHES, WIDTH), jnp.float32), axis=1) * (1.0 / math.sqrt(PATCHES))
    noise = jax.random.normal(noise_key, (BATCH, FRAMES, PATCHES, WIDTH), jnp.float32)
    latents = (time_walk[:, :, None, :] + space_walk[:, None, :, :] + 0.5 * noise).astype(jnp.bfloat16)
    weight_keys = jax.random.split(jax.random.key(seed + 1), 5)
    norm_base = jnp.array([1.0, 0.0, 1.0, 0.0], jnp.float32)
    norms = norm_base[None, :, None] + 0.3 * jax.random.normal(weight_keys[0], (BLOCKS, 4, WIDTH), jnp.float32)
    qkv_gain = jnp.array([1.2, 1.2, 1.0], jnp.float32)[None, None, :, None, None]
    w_qkv = (jax.random.normal(weight_keys[1], (BLOCKS, WIDTH, 3, HEADS, HEAD_DIM), jnp.float32) * qkv_gain / math.sqrt(WIDTH)).astype(jnp.bfloat16)
    w_out = (jax.random.normal(weight_keys[2], (BLOCKS, HEADS, HEAD_DIM, WIDTH), jnp.float32) / math.sqrt(WIDTH)).astype(jnp.bfloat16)
    w_up = (jax.random.normal(weight_keys[3], (BLOCKS, WIDTH, HIDDEN), jnp.float32) / math.sqrt(WIDTH)).astype(jnp.bfloat16)
    w_down = (jax.random.normal(weight_keys[4], (BLOCKS, HIDDEN, WIDTH), jnp.float32) / math.sqrt(HIDDEN)).astype(jnp.bfloat16)
    return {'latents': latents, 'norms': norms, 'w_qkv': w_qkv, 'w_out': w_out, 'w_up': w_up, 'w_down': w_down}


def layer_norm(tokens, norm_gain, norm_shift):
    tokens_f32 = tokens.astype(jnp.float32)
    row_mean = jnp.mean(tokens_f32, axis=-1, keepdims=True)
    centered = tokens_f32 - row_mean
    variance = jnp.mean(jnp.square(centered), axis=-1, keepdims=True)
    return (centered * lax.rsqrt(variance + EPS) * norm_gain + norm_shift).astype(jnp.bfloat16)


def attention(query_rows, key_rows, value_rows, layout):
    seq_axis, score_form, mix_form = layout
    seq_len = query_rows.shape[seq_axis]
    q_block = math.gcd(seq_len, 64)
    logit_scale = HEAD_DIM ** -0.5
    key_f32 = key_rows.astype(jnp.float32)
    value_f32 = value_rows.astype(jnp.float32)

    def attend_block(block_idx, attn_out):
        q_start = block_idx * q_block
        q_part = lax.dynamic_slice_in_dim(query_rows, q_start, q_block, axis=seq_axis).astype(jnp.float32)
        logits = jnp.einsum(score_form, q_part, key_f32) * logit_scale
        attn_probs = jax.nn.softmax(logits, axis=-1).astype(jnp.bfloat16).astype(jnp.float32)
        block_out = jnp.einsum(mix_form, attn_probs, value_f32).astype(jnp.bfloat16)
        return lax.dynamic_update_slice_in_dim(attn_out, block_out, q_start, axis=seq_axis)

    return lax.fori_loop(0, seq_len // q_block, attend_block, jnp.zeros_like(query_rows))


def project_heads(normed, head_weight):
    return jnp.einsum('btsd,dhe->btshe', normed.astype(jnp.float32), head_weight.astype(jnp.float32)).astype(jnp.bfloat16)


def transformer_block(tokens, norm_rows, qkv_weight, out_weight, up_weight, down_weight, layout):
    normed = layer_norm(tokens, norm_rows[0], norm_rows[1])
    mixed_heads = attention(project_heads(normed, qkv_weight[:, 0]), project_heads(normed, qkv_weight[:, 1]), project_heads(normed, qkv_weight[:, 2]), layout)
    attn_proj = jnp.einsum('btshe,hed->btsd', mixed_heads.astype(jnp.float32), out_weight.astype(jnp.float32))
    residual = (tokens.astype(jnp.float32) + attn_proj).astype(jnp.bfloat16)
    normed_mlp = layer_norm(residual, norm_rows[2], norm_rows[3])
    up_proj = jnp.einsum('btsd,df->btsf', normed_mlp.astype(jnp.float32), up_weight.astype(jnp.float32))
    hidden = jax.nn.gelu(up_proj, approximate=True).astype(jnp.bfloat16)
    down_proj = jnp.einsum('btsf,fd->btsd', hidden.astype(jnp.float32), down_weight.astype(jnp.float32))
    return (residual.astype(jnp.float32) + down_proj).astype(jnp.bfloat16)


def reference(latents, norms, w_qkv, w_out, w_up, w_down):
    tokens = latents
    for layer_idx in range(BLOCKS):
        layout = SPATIAL if layer_idx % 2 == 0 else TEMPORAL
        tokens = transformer_block(tokens, norms[layer_idx], w_qkv[layer_idx], w_out[layer_idx], w_up[layer_idx], w_down[layer_idx], layout)
    return tokens
```

```python
import functools
import math

import jax
import jax.numpy as jnp
from jax import lax
from jax.experimental import pallas as pl
from jax.experimental.pallas import tpu as pltpu
from jax.sharding import PartitionSpec as P

EPS = 1e-6
D = 384
QKV = 3 * D
HID = 4 * D
DEV = 128
BLOCKS = 4
CHUNKS = 2
SLOTS = DEV // CHUNKS
ROWS = 4 * SLOTS
HALF = ROWS // 2
EXP_SCALE = 64 ** -0.5 * math.log2(math.e)
GELU_A = math.sqrt(2.0 / math.pi)
GELU_B = GELU_A * 0.044715
BF = jnp.bfloat16
F32 = jnp.float32


def slot_table():
    hops = (0, 1, 2, 1)
    offs = [(z, y, x, c) for z in range(4) for y in range(4) for x in range(4) for c in range(2)]
    offs.sort(key=lambda o: (-(hops[o[0]] + hops[o[1]] + hops[o[2]]), -o[3], o))
    index = {o: k for k, o in enumerate(offs)}
    back = [index[((-o[0]) % 4, (-o[1]) % 4, (-o[2]) % 4, o[3])] for o in offs]
    return offs, back


OFFS, BACK = slot_table()


def layer_norm(u, gain, shift):
    mean = jnp.mean(u, axis=-1, keepdims=True)
    cen = u - mean
    var = jnp.mean(cen * cen, axis=-1, keepdims=True)
    return (cen * lax.rsqrt(var + EPS) * gain + shift).astype(BF)


def gelu(x):
    half = 0.5 * x
    return half + half * jnp.tanh(x * (GELU_A + GELU_B * (x * x)))


def put(ref, start, rows):
    for t in range(3):
        ref[t, pl.ds(start, SLOTS, stride=4), :] = rows[:, t * 128:(t + 1) * 128]


def take(ref, start):
    return jnp.concatenate([ref[t, pl.ds(start, SLOTS, stride=4), :] for t in range(3)], axis=1)


def dot(a, b):
    return jnp.dot(a, b, preferred_element_type=F32)


def stack_kernel(x_ref, tab_ref, norms_ref, wqkv_ref, wout_ref, wup_ref, wdown_ref, y_ref,
                 xv, wqkv, wout, wup, wdown, f_in, f_out, qkv_s, o_s, hid_s, zsend, recv,
                 x_sem, w_sem, send_sem, recv_sem, y_sem):
    me = lax.axis_index('sp')
    digits = (me // 32, (me // 8) % 4, (me // 2) % 4, me % 2)

    barrier = pltpu.get_barrier_semaphore()

    def greet(i, carry):
        pl.semaphore_signal(barrier, inc=1, device_id={'sp': lax.rem(me + i, DEV)}, device_id_type=pl.DeviceIdType.MESH)
        return carry

    x_copy = pltpu.make_async_copy(x_ref, xv, x_sem)
    x_copy.start()
    w_copies = []
    for l in range(BLOCKS):
        row = []
        for i, (src, dst) in enumerate(((wqkv_ref, wqkv), (wout_ref, wout), (wup_ref, wup), (wdown_ref, wdown))):
            cp = pltpu.make_async_copy(src.at[l], dst.at[l], w_sem.at[l, i])
            cp.start()
            row.append(cp)
        w_copies.append(row)
    lax.fori_loop(1, DEV, greet, 0)

    zpos = [(((digits[0] - d) + 4) % 4) * 32 for d in range(4)]
    ypos = [(((digits[1] - d) + 4) % 4) * 8 for d in range(4)]
    xpos = [(((digits[2] - d) + 4) % 4) * 2 for d in range(4)]
    cpos = [(digits[3] + d) % 2 for d in range(2)]

    def dev_of(k):
        o = OFFS[k]
        return zpos[o[0]] + ypos[o[1]] + xpos[o[2]] + cpos[o[3]]

    x_copy.wait()
    lane = lax.broadcasted_iota(jnp.int32, (HALF, 2 * DEV), 1)
    for c in range(CHUNKS):
        tab = tab_ref[c]
        dz = (digits[0] - tab[:, 0:1] + 4) % 4
        dy = (digits[1] - tab[:, 1:2] + 4) % 4
        dx = (digits[2] - tab[:, 2:3] + 4) % 4
        dc = (digits[3] + tab[:, 3:4]) % 2
        patch = 2 * (dz * 32 + dy * 8 + dx * 2 + dc) + tab[:, 4:5]
        pick = jnp.where(lane == patch, 1.0, 0.0).astype(BF)
        for a in range(2):
            rows = dot(pick, xv[a])
            for b in range(2):
                put(f_in, c * ROWS + 2 * a + b, rows[b * SLOTS:(b + 1) * SLOTS])

    low = lax.broadcasted_iota(jnp.int32, (HALF, 128), 1) < 64

    def load_rows(c):
        return jnp.concatenate([take(f_in, c * ROWS + 2 * j + i) for j in range(2) for i in range(2)], axis=0)

    for l in range(BLOCKS):
        gains = norms_ref[l]
        for c in range(CHUNKS):
            if l > 0:
                n = SLOTS - (c == CHUNKS - 1)
                got = recv.at[l - 1, pl.ds(c * SLOTS, n)]
                pltpu.make_async_copy(got, got, recv_sem.at[l - 1, c]).wait()
                if c == CHUNKS - 1:
                    recv[l - 1, DEV - 1] = zsend[l - 1, DEV - 1]
                rows = recv[l - 1, c * SLOTS:(c + 1) * SLOTS].reshape(ROWS, D).astype(F32)
                for t in range(3):
                    f_in[t, c * ROWS:(c + 1) * ROWS, :] = rows[:, t * 128:(t + 1) * 128]
            if c == 0:
                w_copies[l][0].wait()
            normed = layer_norm(load_rows(c), gains[0:1], gains[1:2])
            proj = dot(normed, wqkv[l]).astype(BF)
            for j in range(2):
                qkv_s[j, c * HALF:(c + 1) * HALF, :] = proj[j * HALF:(j + 1) * HALF]
        for c in range(CHUNKS):
            for j in range(2):
                for t in range(3):
                    q = qkv_s[j, c * HALF:(c + 1) * HALF, t * 128:(t + 1) * 128]
                    k = qkv_s[j, :, D + t * 128:D + (t + 1) * 128]
                    v = qkv_s[j, :, 2 * D + t * 128:2 * D + (t + 1) * 128]
                    zero = jnp.zeros_like(q)
                    qq = jnp.concatenate([jnp.where(low, q, zero), jnp.where(low, zero, q)], axis=0)
                    s = lax.dot_general(qq, k, (((1,), (1,)), ((), ())), preferred_element_type=F32)
                    e = jnp.exp2((s - jnp.max(s, axis=-1, keepdims=True)) * EXP_SCALE)
                    p = (e * (1.0 / jnp.sum(e, axis=-1, keepdims=True))).astype(BF)
                    oo = dot(p, v)
                    o_s[j * HALF:(j + 1) * HALF, t * 128:(t + 1) * 128] = jnp.where(low, oo[:HALF], oo[HALF:]).astype(BF)
            if c == 0:
                for cp in w_copies[l][1:]:
                    cp.wait()
            h = (load_rows(c) + dot(o_s[...], wout[l])).astype(BF).astype(F32)
            normed = layer_norm(h, gains[2:3], gains[3:4])
            for n in range(0, HID, 512):
                hid_s[:, n:n + 512] = gelu(dot(normed, wup[l, :, n:n + 512])).astype(BF)
            z = h + dot(hid_s[...], wdown[l])
            for j in range(2):
                for b in range(2):
                    put(f_out, 2 * b + j, z[(2 * j + b) * SLOTS:(2 * j + b + 1) * SLOTS])
            zs = jnp.concatenate([f_out[t] for t in range(3)], axis=1)
            zsend[l, c * SLOTS:(c + 1) * SLOTS] = zs.astype(BF).reshape(SLOTS, 4, D)
            if l == 0 and c == 0:
                pl.semaphore_wait(barrier, DEV - 1)
            for k in range(c * SLOTS, (c + 1) * SLOTS):
                if l == BLOCKS - 1:
                    pltpu.make_async_copy(zsend.at[l, k], y_ref.at[dev_of(k)], y_sem).start()
                elif k < DEV - 1:
                    pltpu.make_async_remote_copy(zsend.at[l, k], recv.at[l, BACK[k]], send_sem.at[l, c], recv_sem.at[l, c],
                                                 device_id={'sp': dev_of(k)}, device_id_type=pl.DeviceIdType.MESH).start()

    for l in range(BLOCKS - 1):
        for c in range(CHUNKS):
            n = SLOTS - (c == CHUNKS - 1)
            sent = zsend.at[l, pl.ds(c * SLOTS, n)]
            pltpu.make_async_copy(sent, sent, send_sem.at[l, c]).wait()
    pltpu.make_async_copy(zsend.at[BLOCKS - 1], y_ref, y_sem).wait()


def solution(mesh):
    table = [[list(OFFS[c * SLOTS + r % SLOTS]) + [r // SLOTS] for r in range(HALF)] for c in range(CHUNKS)]

    def local_stack(latents, norms, w_qkv, w_out, w_up, w_down):
        anywhere = pl.BlockSpec(memory_space=pl.ANY)
        vmem = pl.BlockSpec(memory_space=pltpu.VMEM)
        out = pl.pallas_call(
            stack_kernel,
            out_shape=jax.ShapeDtypeStruct((DEV, 4, D), BF),
            in_specs=[anywhere, vmem, vmem, anywhere, anywhere, anywhere, anywhere],
            out_specs=anywhere,
            scratch_shapes=[
                pltpu.VMEM((2, 2 * DEV, D), BF),
                pltpu.VMEM((BLOCKS, D, QKV), BF),
                pltpu.VMEM((BLOCKS, D, D), BF),
                pltpu.VMEM((BLOCKS, D, HID), BF),
                pltpu.VMEM((BLOCKS, HID, D), BF),
                pltpu.VMEM((3, 4 * DEV, 128), F32),
                pltpu.VMEM((3, ROWS, 128), F32),
                pltpu.VMEM((2, 2 * DEV, QKV), BF),
                pltpu.VMEM((ROWS, D), BF),
                pltpu.VMEM((ROWS, HID), BF),
                pltpu.VMEM((BLOCKS, DEV, 4, D), BF),
                pltpu.VMEM((BLOCKS - 1, DEV, 4, D), BF),
                pltpu.SemaphoreType.DMA,
                pltpu.SemaphoreType.DMA((BLOCKS, 4)),
                pltpu.SemaphoreType.DMA((BLOCKS - 1, CHUNKS)),
                pltpu.SemaphoreType.DMA((BLOCKS - 1, CHUNKS)),
                pltpu.SemaphoreType.DMA,
            ],
            compiler_params=pltpu.CompilerParams(collective_id=0, has_side_effects=True, vmem_limit_bytes=60 * 1024 * 1024),
            name='stack',
        )(latents.reshape(2, 2 * DEV, D), jnp.asarray(table, jnp.int32), norms, w_qkv.reshape(BLOCKS, D, QKV),
          w_out.reshape(BLOCKS, D, D), w_up, w_down)
        return out.reshape(1, 2 * DEV, 2, D)

    replicated = P()
    return jax.shard_map(local_stack, mesh=mesh, in_specs=(P('data', 'sp', None, None), replicated, replicated, replicated, replicated, replicated), out_specs=P('data', None, 'sp', None), check_vma=False)
```

```python
import functools
import math

import jax
import jax.numpy as jnp
from jax import lax
from jax.experimental import pallas as pl
from jax.experimental.pallas import tpu as pltpu
from jax.sharding import PartitionSpec as P

EPS = 1e-6
D = 384
QKV = 3 * D
HID = 4 * D
DEV = 128
BLOCKS = 4
CHUNKS = 2
SLOTS = DEV // CHUNKS
ROWS = 4 * SLOTS
HALF = ROWS // 2
EXP_SCALE = 64 ** -0.5 * math.log2(math.e)
GELU_A = math.sqrt(2.0 / math.pi)
GELU_B = GELU_A * 0.044715
BF = jnp.bfloat16
F32 = jnp.float32


def slot_table():
    hops = (0, 1, 2, 1)
    offs = [(z, y, x, c) for z in range(4) for y in range(4) for x in range(4) for c in range(2)]
    offs.sort(key=lambda o: (-(hops[o[0]] + hops[o[1]] + hops[o[2]]), -o[3], o))
    index = {o: k for k, o in enumerate(offs)}
    back = [index[((-o[0]) % 4, (-o[1]) % 4, (-o[2]) % 4, o[3])] for o in offs]
    return offs, back


OFFS, BACK = slot_table()


def layer_norm(u, gain, shift):
    mean = jnp.mean(u, axis=-1, keepdims=True)
    cen = u - mean
    var = jnp.mean(cen * cen, axis=-1, keepdims=True)
    return (cen * lax.rsqrt(var + EPS) * gain + shift).astype(BF)


def gelu(x):
    half = 0.5 * x
    return half + half * jnp.tanh(x * (GELU_A + GELU_B * (x * x)))


def put(ref, start, rows):
    for t in range(3):
        ref[t, pl.ds(start, SLOTS, stride=4), :] = rows[:, t * 128:(t + 1) * 128]


def take(ref, start):
    return jnp.concatenate([ref[t, pl.ds(start, SLOTS, stride=4), :] for t in range(3)], axis=1)


def dot(a, b):
    return jnp.dot(a, b, preferred_element_type=F32)


def stack_kernel(x_ref, tab_ref, norms_ref, wqkv_ref, wout_ref, wup_ref, wdown_ref, y_ref,
                 xv, wqkv, wout, wup, wdown, f_in, f_out, a_s, qkv_s, o_s, hid_s, zfin, zsend, recv,
                 x_sem, w_sem, send_sem, recv_sem, y_sem):
    me = lax.axis_index('sp')
    digits = (me // 32, (me // 8) % 4, (me // 2) % 4, me % 2)

    barrier = pltpu.get_barrier_semaphore()

    def greet(i, carry):
        pl.semaphore_signal(barrier, inc=1, device_id={'sp': lax.rem(me + i, DEV)}, device_id_type=pl.DeviceIdType.MESH)
        return carry

    x_copy = pltpu.make_async_copy(x_ref, xv, x_sem)
    x_copy.start()
    w_copies = []
    for l in range(BLOCKS):
        row = []
        for i, (src, dst) in enumerate(((wqkv_ref, wqkv), (wout_ref, wout), (wup_ref, wup), (wdown_ref, wdown))):
            cp = pltpu.make_async_copy(src.at[l], dst.at[l], w_sem.at[l, i])
            cp.start()
            row.append(cp)
        w_copies.append(row)
    lax.fori_loop(1, DEV, greet, 0)

    zpos = [(((digits[0] - d) + 4) % 4) * 32 for d in range(4)]
    ypos = [(((digits[1] - d) + 4) % 4) * 8 for d in range(4)]
    xpos = [(((digits[2] - d) + 4) % 4) * 2 for d in range(4)]
    cpos = [(digits[3] + d) % 2 for d in range(2)]

    def dev_of(k):
        o = OFFS[k]
        return zpos[o[0]] + ypos[o[1]] + xpos[o[2]] + cpos[o[3]]

    x_copy.wait()
    lane = lax.broadcasted_iota(jnp.int32, (HALF, 2 * DEV), 1)
    for c in range(CHUNKS):
        tab = tab_ref[c]
        dz = (digits[0] - tab[:, 0:1] + 4) % 4
        dy = (digits[1] - tab[:, 1:2] + 4) % 4
        dx = (digits[2] - tab[:, 2:3] + 4) % 4
        dc = (digits[3] + tab[:, 3:4]) % 2
        patch = 2 * (dz * 32 + dy * 8 + dx * 2 + dc) + tab[:, 4:5]
        pick = jnp.where(lane == patch, 1.0, 0.0).astype(BF)
        for a in range(2):
            rows = dot(pick, xv[a])
            for b in range(2):
                put(f_in, c * ROWS + 2 * a + b, rows[b * SLOTS:(b + 1) * SLOTS])

    low = lax.broadcasted_iota(jnp.int32, (2 * DEV, 128), 1) < 64

    def load_rows(c):
        return jnp.concatenate([take(f_in, c * ROWS + 2 * j + i) for j in range(2) for i in range(2)], axis=0)

    for l in range(BLOCKS):
        gains = norms_ref[l]
        for c in range(CHUNKS):
            if l > 0:
                n = SLOTS - (c == CHUNKS - 1)
                got = recv.at[l - 1, pl.ds(c * SLOTS, n)]
                pltpu.make_async_copy(got, got, recv_sem.at[l - 1, c]).wait()
                if c == CHUNKS - 1:
                    recv[l - 1, DEV - 1] = zsend[l - 1, DEV - 1]
                rows = recv[l - 1, c * SLOTS:(c + 1) * SLOTS].reshape(ROWS, D).astype(F32)
                for t in range(3):
                    f_in[t, c * ROWS:(c + 1) * ROWS, :] = rows[:, t * 128:(t + 1) * 128]
            normed = layer_norm(load_rows(c), gains[0:1], gains[1:2])
            for j in range(2):
                a_s[j, c * HALF:(c + 1) * HALF, :] = normed[j * HALF:(j + 1) * HALF]
        w_copies[l][0].wait()
        normed = a_s[...].reshape(4 * DEV, D)
        for n in range(0, QKV, 384):
            proj = lax.dot_general(normed, wqkv[l, n:n + 384], (((1,), (1,)), ((), ())), preferred_element_type=F32)
            qkv_s[:, :, n:n + 384] = proj.astype(BF).reshape(2, 2 * DEV, 384)
        for j in range(2):
            for t in range(3):
                q = qkv_s[j, :, t * 128:(t + 1) * 128]
                k = qkv_s[j, :, D + t * 128:D + (t + 1) * 128]
                v = qkv_s[j, :, 2 * D + t * 128:2 * D + (t + 1) * 128]
                zero = jnp.zeros_like(q)
                qq = jnp.concatenate([jnp.where(low, q, zero), jnp.where(low, zero, q)], axis=0)
                s = lax.dot_general(qq, k, (((1,), (1,)), ((), ())), preferred_element_type=F32)
                e = jnp.exp2((s - jnp.max(s, axis=-1, keepdims=True)) * EXP_SCALE)
                p = (e * (1.0 / jnp.sum(e, axis=-1, keepdims=True))).astype(BF)
                oo = dot(p, v)
                o_s[j, :, t * 128:(t + 1) * 128] = jnp.where(low, oo[:2 * DEV], oo[2 * DEV:]).astype(BF)
        for c in range(CHUNKS):
            if c == 0:
                for cp in w_copies[l][1:]:
                    cp.wait()
            h = (load_rows(c) + dot(o_s[:, c * HALF:(c + 1) * HALF, :].reshape(ROWS, D), wout[l])).astype(BF).astype(F32)
            normed = layer_norm(h, gains[2:3], gains[3:4])
            for n in range(0, HID, 512):
                hid_s[:, n:n + 512] = gelu(dot(normed, wup[l, :, n:n + 512])).astype(BF)
            z = h + dot(hid_s[...], wdown[l])
            for j in range(2):
                for b in range(2):
                    put(f_out, 2 * b + j, z[(2 * j + b) * SLOTS:(2 * j + b + 1) * SLOTS])
            zs = jnp.concatenate([f_out[t] for t in range(3)], axis=1)
            if l == BLOCKS - 1:
                zfin[c * SLOTS:(c + 1) * SLOTS] = zs.astype(BF).reshape(SLOTS, 2, 2, D)
            else:
                zsend[l, c * SLOTS:(c + 1) * SLOTS] = zs.astype(BF).reshape(SLOTS, 4, D)
            if l == 0 and c == 0:
                pl.semaphore_wait(barrier, DEV - 1)
            for k in range(c * SLOTS, (c + 1) * SLOTS):
                if l == BLOCKS - 1:
                    pltpu.make_async_copy(zfin.at[k], y_ref.at[dev_of(k)], y_sem).start()
                elif k < DEV - 1:
                    pltpu.make_async_remote_copy(zsend.at[l, k], recv.at[l, BACK[k]], send_sem.at[l, c], recv_sem.at[l, c],
                                                 device_id={'sp': dev_of(k)}, device_id_type=pl.DeviceIdType.MESH).start()

    for l in range(BLOCKS - 1):
        for c in range(CHUNKS):
            n = SLOTS - (c == CHUNKS - 1)
            sent = zsend.at[l, pl.ds(c * SLOTS, n)]
            pltpu.make_async_copy(sent, sent, send_sem.at[l, c]).wait()
    pltpu.make_async_copy(zfin, y_ref, y_sem).wait()


def solution(mesh):
    table = [[list(OFFS[c * SLOTS + r % SLOTS]) + [r // SLOTS] for r in range(HALF)] for c in range(CHUNKS)]

    def local_stack(latents, norms, w_qkv, w_out, w_up, w_down):
        anywhere = pl.BlockSpec(memory_space=pl.ANY)
        vmem = pl.BlockSpec(memory_space=pltpu.VMEM)
        out = pl.pallas_call(
            stack_kernel,
            out_shape=jax.ShapeDtypeStruct((DEV, 2, 2, D), BF),
            in_specs=[anywhere, vmem, vmem, anywhere, anywhere, anywhere, anywhere],
            out_specs=anywhere,
            scratch_shapes=[
                pltpu.VMEM((2, 2 * DEV, D), BF),
                pltpu.VMEM((BLOCKS, QKV, D), BF),
                pltpu.VMEM((BLOCKS, D, D), BF),
                pltpu.VMEM((BLOCKS, D, HID), BF),
                pltpu.VMEM((BLOCKS, HID, D), BF),
                pltpu.VMEM((3, 4 * DEV, 128), F32),
                pltpu.VMEM((3, ROWS, 128), F32),
                pltpu.VMEM((2, 2 * DEV, D), BF),
                pltpu.VMEM((2, 2 * DEV, QKV), BF),
                pltpu.VMEM((2, 2 * DEV, D), BF),
                pltpu.VMEM((ROWS, HID), BF),
                pltpu.VMEM((DEV, 2, 2, D), BF),
                pltpu.VMEM((BLOCKS - 1, DEV, 4, D), BF),
                pltpu.VMEM((BLOCKS - 1, DEV, 4, D), BF),
                pltpu.SemaphoreType.DMA,
                pltpu.SemaphoreType.DMA((BLOCKS, 4)),
                pltpu.SemaphoreType.DMA((BLOCKS - 1, CHUNKS)),
                pltpu.SemaphoreType.DMA((BLOCKS - 1, CHUNKS)),
                pltpu.SemaphoreType.DMA,
            ],
            compiler_params=pltpu.CompilerParams(collective_id=0, has_side_effects=True, vmem_limit_bytes=60 * 1024 * 1024),
            name='stack',
        )(latents.reshape(2, 2 * DEV, D), jnp.asarray(table, jnp.int32), norms, jnp.transpose(w_qkv, (0, 2, 3, 4, 1)).reshape(BLOCKS, QKV, D),
          w_out.reshape(BLOCKS, D, D), w_up, w_down)
        return out.reshape(1, 2 * DEV, 2, D)

    replicated = P()
    return jax.shard_map(local_stack, mesh=mesh, in_specs=(P('data', 'sp', None, None), replicated, replicated, replicated, replicated, replicated), out_specs=P('data', None, 'sp', None), check_vma=False)
```

```python
import math

import jax
import jax.numpy as jnp
from jax import lax
from jax.experimental import pallas as pl
from jax.experimental.pallas import tpu as pltpu
from jax.sharding import PartitionSpec as P

EPS = 1e-6
D = 384
QKV = 3 * D
HID = 4 * D
DEV = 128
SEQ = 2 * DEV
BLOCKS = 4
CUTS = (0, 64, 128)
CHUNKS = tuple((a, b - a) for a, b in zip(CUTS, CUTS[1:]))
BIG = max(n for _, n in CHUNKS)
UP = 256
EXP_SCALE = 64 ** -0.5 * math.log2(math.e)
GELU_A = math.sqrt(2.0 / math.pi)
GELU_B = GELU_A * 0.044715
BF = jnp.bfloat16
F32 = jnp.float32


def slot_table():
    hops = (0, 1, 2, 1)
    offs = [(z, y, x, c) for z in range(4) for y in range(4) for x in range(4) for c in range(2)]

    def opposite(o):
        return (-o[0]) % 4, (-o[1]) % 4, (-o[2]) % 4, o[3]

    offs.sort(key=lambda o: (-(hops[o[0]] + hops[o[1]] + hops[o[2]]), -o[3], min(o, opposite(o)), o))
    index = {o: k for k, o in enumerate(offs)}
    back = [index[opposite(o)] for o in offs]
    assert all(start <= back[k] < start + n for start, n in CHUNKS for k in range(start, start + n))
    return offs, back


OFFS, BACK = slot_table()


def layer_norm(u, gain, shift):
    mean = jnp.mean(u, axis=-1, keepdims=True)
    cen = u - mean
    var = jnp.mean(cen * cen, axis=-1, keepdims=True)
    return (cen * lax.rsqrt(var + EPS) * gain + shift).astype(BF)


def gelu(x):
    half = 0.5 * x
    return half + half * jnp.tanh(x * (GELU_A + GELU_B * (x * x)))


def dot(a, b):
    return jnp.dot(a, b, preferred_element_type=F32)


def dot_t(a, b):
    return lax.dot_general(a, b, (((1,), (1,)), ((), ())), preferred_element_type=F32)


def put(ref, start, rows):
    n = rows.shape[0]
    for t in range(3):
        ref[t, pl.ds(start, n, stride=4), :] = rows[:, t * 128:(t + 1) * 128]


def take(ref, start, n):
    return jnp.concatenate([ref[t, pl.ds(start, n, stride=4), :] for t in range(3)], axis=1)


def stack_kernel(x_ref, tab_ref, norms_ref, wqkv_ref, wout_ref, wup_ref, wdown_ref, y_ref,
                 xv, tab, norms, wqkv, wout, wup, wdown, f_in, f_out, a_s, qkv_s, o_s, hid_s, zfin, zsend, recv,
                 in_sem, w_sem, send_sem, recv_sem, y_sem):
    me = lax.axis_index('sp')
    digits = (me // 32, (me // 8) % 4, (me // 2) % 4, me % 2)
    barrier = pltpu.get_barrier_semaphore()

    def greet(i, carry):
        pl.semaphore_signal(barrier, inc=1, device_id={'sp': lax.rem(me + i, DEV)}, device_id_type=pl.DeviceIdType.MESH)
        return carry

    first = [pltpu.make_async_copy(src, dst, in_sem.at[i]) for i, (src, dst) in enumerate(((x_ref, xv), (tab_ref, tab), (norms_ref, norms)))]
    weights = [[pltpu.make_async_copy(src.at[l], dst.at[l], w_sem.at[l, i])
                for i, (src, dst) in enumerate(((wqkv_ref, wqkv), (wout_ref, wout), (wup_ref, wup), (wdown_ref, wdown)))]
               for l in range(BLOCKS)]
    for cp in first:
        cp.start()
    weights[0][0].start()
    lax.fori_loop(1, DEV, greet, 0)

    zpos = [(((digits[0] - d) + 4) % 4) * 32 for d in range(4)]
    ypos = [(((digits[1] - d) + 4) % 4) * 8 for d in range(4)]
    xpos = [(((digits[2] - d) + 4) % 4) * 2 for d in range(4)]
    cpos = [(digits[3] + d) % 2 for d in range(2)]

    def dev_of(k):
        o = OFFS[k]
        return zpos[o[0]] + ypos[o[1]] + xpos[o[2]] + cpos[o[3]]

    def send(l, c, k):
        if l == BLOCKS - 1:
            pltpu.make_async_copy(zfin.at[k], y_ref.at[dev_of(k)], y_sem).start()
        elif k < DEV - 1:
            pltpu.make_async_remote_copy(zsend.at[l, k], recv.at[l, BACK[k]], send_sem.at[l, c], recv_sem.at[l, c],
                                         device_id={'sp': dev_of(k)}, device_id_type=pl.DeviceIdType.MESH).start()

    def load_rows(c):
        start, n = CHUNKS[c]
        return jnp.concatenate([take(f_in, 4 * start + 2 * j + i, n) for j in range(2) for i in range(2)], axis=0)

    for cp in first:
        cp.wait()
    for cp in weights[0][1:]:
        cp.start()
    lane = lax.broadcasted_iota(jnp.int32, (SEQ, SEQ), 1)
    dz = (digits[0] - tab[:, 0:1] + 4) % 4
    dy = (digits[1] - tab[:, 1:2] + 4) % 4
    dx = (digits[2] - tab[:, 2:3] + 4) % 4
    dc = (digits[3] + tab[:, 3:4]) % 2
    patch = 2 * (dz * 32 + dy * 8 + dx * 2 + dc) + tab[:, 4:5]
    pick = jnp.where(lane == patch, 1.0, 0.0).astype(BF)
    for a in range(2):
        rows = dot(pick, xv[a])
        for start, n in CHUNKS:
            for b in range(2):
                put(f_in, 4 * start + 2 * a + b, rows[2 * start + b * n:2 * start + (b + 1) * n])

    low = lax.broadcasted_iota(jnp.int32, (SEQ, 128), 1) < 64

    for l in range(BLOCKS):
        gains = norms[l]
        for c, (start, n) in enumerate(CHUNKS):
            if l > 0:
                last = start + n == DEV
                got = recv.at[l - 1, pl.ds(start, n - last)]
                pltpu.make_async_copy(got, got, recv_sem.at[l - 1, c]).wait()
                if last:
                    recv[l - 1, DEV - 1] = zsend[l - 1, DEV - 1]
                rows = recv[l - 1, start:start + n].reshape(4 * n, D).astype(F32)
                for t in range(3):
                    f_in[t, 4 * start:4 * (start + n), :] = rows[:, t * 128:(t + 1) * 128]
            normed = layer_norm(load_rows(c), gains[0:1], gains[1:2])
            for j in range(2):
                a_s[j, 2 * start:2 * (start + n), :] = normed[2 * j * n:2 * (j + 1) * n]
        weights[l][0].wait()
        normed = a_s[...].reshape(2 * SEQ, D)
        for m in range(0, QKV, 384):
            qkv_s[:, :, m:m + 384] = dot_t(normed, wqkv[l, m:m + 384]).astype(BF).reshape(2, SEQ, 384)
        if l == 0:
            for row in weights[1:]:
                for cp in row:
                    cp.start()
        for j in range(2):
            for t in range(3):
                q = qkv_s[j, :, t * 128:(t + 1) * 128]
                k = qkv_s[j, :, D + t * 128:D + (t + 1) * 128]
                v = qkv_s[j, :, 2 * D + t * 128:2 * D + (t + 1) * 128]
                zero = jnp.zeros_like(q)
                s = dot_t(jnp.concatenate([jnp.where(low, q, zero), jnp.where(low, zero, q)], axis=0), k)
                e = jnp.exp2((s - jnp.max(s, axis=-1, keepdims=True)) * EXP_SCALE)
                p = (e * (1.0 / jnp.sum(e, axis=-1, keepdims=True))).astype(BF)
                oo = dot(p, v)
                o_s[j, :, t * 128:(t + 1) * 128] = jnp.where(low, oo[:SEQ], oo[SEQ:]).astype(BF)
        for cp in weights[l][1:]:
            cp.wait()
        pending = []

        def flush(count):
            for args in pending[:count]:
                send(*args)
            del pending[:count]

        for c, (start, n) in enumerate(CHUNKS):
            share = -(-len(pending) // 7)
            mixed = jnp.concatenate([o_s[j, 2 * start:2 * (start + n), :] for j in range(2)], axis=0)
            h = (load_rows(c) + dot(mixed, wout[l])).astype(BF).astype(F32)
            normed = layer_norm(h, gains[2:3], gains[3:4])
            for m in range(0, HID, UP):
                flush(share)
                hid_s[0:4 * n, m:m + UP] = gelu(dot(normed, wup[l, :, m:m + UP])).astype(BF)
            flush(len(pending))
            z = h + dot(hid_s[0:4 * n], wdown[l])
            for j in range(2):
                for b in range(2):
                    put(f_out, 2 * b + j, z[(2 * j + b) * n:(2 * j + b + 1) * n])
            zs = jnp.concatenate([f_out[t, 0:4 * n] for t in range(3)], axis=1).astype(BF)
            if l == BLOCKS - 1:
                zfin[start:start + n] = zs.reshape(n, 2, 2, D)
            else:
                zsend[l, start:start + n] = zs.reshape(n, 4, D)
            if l == 0 and c == 0:
                pl.semaphore_wait(barrier, DEV - 1)
            pending = [(l, c, k) for k in range(start, start + n)]
        flush(len(pending))

    for l in range(BLOCKS - 1):
        for c, (start, n) in enumerate(CHUNKS):
            sent = zsend.at[l, pl.ds(start, n - (start + n == DEV))]
            pltpu.make_async_copy(sent, sent, send_sem.at[l, c]).wait()
    pltpu.make_async_copy(zfin, y_ref, y_sem).wait()


def solution(mesh):
    table = [list(OFFS[start + r]) + [b] for start, n in CHUNKS for b in range(2) for r in range(n)]

    def local_stack(latents, norms, w_qkv, w_out, w_up, w_down):
        anywhere = pl.BlockSpec(memory_space=pl.ANY)
        dma = pltpu.SemaphoreType.DMA
        out = pl.pallas_call(
            stack_kernel,
            out_shape=jax.ShapeDtypeStruct((DEV, 2, 2, D), BF),
            in_specs=[anywhere] * 7,
            out_specs=anywhere,
            scratch_shapes=[
                pltpu.VMEM((2, SEQ, D), BF),
                pltpu.VMEM((SEQ, 5), jnp.int32),
                pltpu.VMEM((BLOCKS, 4, D), F32),
                pltpu.VMEM((BLOCKS, QKV, D), BF),
                pltpu.VMEM((BLOCKS, D, D), BF),
                pltpu.VMEM((BLOCKS, D, HID), BF),
                pltpu.VMEM((BLOCKS, HID, D), BF),
                pltpu.VMEM((3, 2 * SEQ, 128), F32),
                pltpu.VMEM((3, 4 * BIG, 128), F32),
                pltpu.VMEM((2, SEQ, D), BF),
                pltpu.VMEM((2, SEQ, QKV), BF),
                pltpu.VMEM((2, SEQ, D), BF),
                pltpu.VMEM((4 * BIG, HID), BF),
                pltpu.VMEM((DEV, 2, 2, D), BF),
                pltpu.VMEM((BLOCKS - 1, DEV, 4, D), BF),
                pltpu.VMEM((BLOCKS - 1, DEV, 4, D), BF),
                dma((3,)),
                dma((BLOCKS, 4)),
                dma((BLOCKS - 1, len(CHUNKS))),
                dma((BLOCKS - 1, len(CHUNKS))),
                dma,
            ],
            compiler_params=pltpu.CompilerParams(collective_id=0, has_side_effects=True, vmem_limit_bytes=60 * 1024 * 1024),
            name='stack',
        )(latents.reshape(2, SEQ, D), jnp.asarray(table, jnp.int32), norms, jnp.transpose(w_qkv, (0, 2, 3, 4, 1)).reshape(BLOCKS, QKV, D),
          w_out.reshape(BLOCKS, D, D), w_up, w_down)
        return out.reshape(1, SEQ, 2, D)

    replicated = P()
    return jax.shard_map(local_stack, mesh=mesh, in_specs=(P('data', 'sp', None, None), replicated, replicated, replicated, replicated, replicated), out_specs=P('data', None, 'sp', None), check_vma=False)
```

```python
import math

import jax
import jax.numpy as jnp
from jax import lax
from jax.experimental import pallas as pl
from jax.experimental.pallas import tpu as pltpu
from jax.sharding import PartitionSpec as P

EPS = 1e-6
D = 384
QKV = 3 * D
HID = 4 * D
DEV = 128
SEQ = 2 * DEV
BLOCKS = 4
CUTS = (0, 64, 128)
CHUNKS = tuple((a, b - a) for a, b in zip(CUTS, CUTS[1:]))
BIG = max(n for _, n in CHUNKS)
UP = 512
EXP_SCALE = 64 ** -0.5 * math.log2(math.e)
GELU_A = math.sqrt(2.0 / math.pi)
GELU_B = GELU_A * 0.044715
BF = jnp.bfloat16
F32 = jnp.float32


def slot_table():
    hops = (0, 1, 2, 1)
    offs = [(z, y, x, c) for z in range(4) for y in range(4) for x in range(4) for c in range(2)]

    def opposite(o):
        return (-o[0]) % 4, (-o[1]) % 4, (-o[2]) % 4, o[3]

    offs.sort(key=lambda o: (-(hops[o[0]] + hops[o[1]] + hops[o[2]]), -o[3], min(o, opposite(o)), o))
    index = {o: k for k, o in enumerate(offs)}
    back = [index[opposite(o)] for o in offs]
    assert all(start <= back[k] < start + n for start, n in CHUNKS for k in range(start, start + n))
    return offs, back


OFFS, BACK = slot_table()


def layer_norm(u, gain, shift):
    mean = jnp.mean(u, axis=-1, keepdims=True)
    cen = u - mean
    var = jnp.mean(cen * cen, axis=-1, keepdims=True)
    return (cen * lax.rsqrt(var + EPS) * gain + shift).astype(BF)


def gelu(x):
    half = 0.5 * x
    return half + half * jnp.tanh(x * (GELU_A + GELU_B * (x * x)))


def dot(a, b):
    return jnp.dot(a, b, preferred_element_type=F32)


def dot_t(a, b):
    return lax.dot_general(a, b, (((1,), (1,)), ((), ())), preferred_element_type=F32)


def put(ref, start, rows):
    n = rows.shape[0]
    for t in range(3):
        ref[t, pl.ds(start, n, stride=4), :] = rows[:, t * 128:(t + 1) * 128]


def take(ref, start, n):
    return jnp.concatenate([ref[t, pl.ds(start, n, stride=4), :] for t in range(3)], axis=1)


def stack_kernel(x_ref, tab_ref, norms_ref, wqkv_ref, wout_ref, wup_ref, wdown_ref, y_ref,
                 xv, tab, norms, wqkv, wout, wup, wdown, wq_s, f_in, f_out, a_s, qkv_s, o_s, hid_s, zfin, zsend, recv,
                 in_sem, w_sem, send_sem, recv_sem, y_sem):
    me = lax.axis_index('sp')
    digits = (me // 32, (me // 8) % 4, (me // 2) % 4, me % 2)
    barrier = pltpu.get_barrier_semaphore()

    def greet(i, carry):
        pl.semaphore_signal(barrier, inc=1, device_id={'sp': lax.rem(me + i, DEV)}, device_id_type=pl.DeviceIdType.MESH)
        return carry

    first = [pltpu.make_async_copy(src, dst, in_sem.at[i]) for i, (src, dst) in enumerate(((x_ref, xv), (tab_ref, tab), (norms_ref, norms)))]
    weights = [[pltpu.make_async_copy(src.at[l], dst.at[l], w_sem.at[l, i])
                for i, (src, dst) in enumerate(((wqkv_ref, wqkv), (wout_ref, wout), (wup_ref, wup), (wdown_ref, wdown)))]
               for l in range(BLOCKS)]
    for cp in first:
        cp.start()
    weights[0][0].start()
    lax.fori_loop(1, DEV, greet, 0)

    zpos = [(((digits[0] - d) + 4) % 4) * 32 for d in range(4)]
    ypos = [(((digits[1] - d) + 4) % 4) * 8 for d in range(4)]
    xpos = [(((digits[2] - d) + 4) % 4) * 2 for d in range(4)]
    cpos = [(digits[3] + d) % 2 for d in range(2)]

    def dev_of(k):
        o = OFFS[k]
        return zpos[o[0]] + ypos[o[1]] + xpos[o[2]] + cpos[o[3]]

    def send(l, c, k):
        if l == BLOCKS - 1:
            pltpu.make_async_copy(zfin.at[k], y_ref.at[dev_of(k)], y_sem).start()
        elif k < DEV - 1:
            pltpu.make_async_remote_copy(zsend.at[l, k], recv.at[l, BACK[k]], send_sem.at[l, c], recv_sem.at[l, c],
                                         device_id={'sp': dev_of(k)}, device_id_type=pl.DeviceIdType.MESH).start()

    def load_rows(c):
        start, n = CHUNKS[c]
        return jnp.concatenate([take(f_in, 4 * start + 2 * j + i, n) for j in range(2) for i in range(2)], axis=0)

    for cp in first:
        cp.wait()
    for cp in weights[0][1:]:
        cp.start()
    lane = lax.broadcasted_iota(jnp.int32, (SEQ, SEQ), 1)
    dz = (digits[0] - tab[:, 0:1] + 4) % 4
    dy = (digits[1] - tab[:, 1:2] + 4) % 4
    dx = (digits[2] - tab[:, 2:3] + 4) % 4
    dc = (digits[3] + tab[:, 3:4]) % 2
    patch = 2 * (dz * 32 + dy * 8 + dx * 2 + dc) + tab[:, 4:5]
    pick = jnp.where(lane == patch, 1.0, 0.0).astype(BF)
    for a in range(2):
        rows = dot(pick, xv[a])
        for start, n in CHUNKS:
            for b in range(2):
                put(f_in, 4 * start + 2 * a + b, rows[2 * start + b * n:2 * start + (b + 1) * n])

    pending = []

    def flush(count):
        for args in pending[:count]:
            send(*args)
        del pending[:count]

    def lay_out(l):
        for m in range(0, QKV, 384):
            wq_s[:, m:m + 384] = wqkv[l, m:m + 384].T

    weights[0][0].wait()
    lay_out(0)
    for l in range(BLOCKS):
        gains = norms[l]
        for c, (start, n) in enumerate(CHUNKS):
            if l > 0:
                last = start + n == DEV
                got = recv.at[l - 1, pl.ds(start, n - last)]
                pltpu.make_async_copy(got, got, recv_sem.at[l - 1, c]).wait()
                if last:
                    recv[l - 1, DEV - 1] = zsend[l - 1, DEV - 1]
                rows = recv[l - 1, start:start + n].reshape(4 * n, D).astype(F32)
                for t in range(3):
                    f_in[t, 4 * start:4 * (start + n), :] = rows[:, t * 128:(t + 1) * 128]
            normed = layer_norm(load_rows(c), gains[0:1], gains[1:2])
            for j in range(2):
                a_s[j, 2 * start:2 * (start + n), :] = normed[2 * j * n:2 * (j + 1) * n]
            if (start + n) % 64 == 0:
                r = 2 * (start + n) - 128
                normed = a_s[:, r:r + 128].reshape(256, D)
                for m in range(0, QKV, 384):
                    qkv_s[:, r:r + 128, m:m + 384] = dot(normed, wq_s[:, m:m + 384]).astype(BF).reshape(2, 128, 384)
        if l == 0:
            for row in weights[1:]:
                for cp in row:
                    cp.start()
        for c, (start, n) in enumerate(CHUNKS):
            low = lax.broadcasted_iota(jnp.int32, (2 * n, 128), 1) < 64
            share = len(pending)
            for j in range(2):
                for t in range(3):
                    flush(share)
                    q = qkv_s[j, 2 * start:2 * (start + n), t * 128:(t + 1) * 128]
                    k = qkv_s[j, :, D + t * 128:D + (t + 1) * 128]
                    v = qkv_s[j, :, 2 * D + t * 128:2 * D + (t + 1) * 128]
                    zero = jnp.zeros_like(q)
                    s = dot_t(jnp.concatenate([jnp.where(low, q, zero), jnp.where(low, zero, q)], axis=0), k)
                    e = jnp.exp2((s - jnp.max(s, axis=-1, keepdims=True)) * EXP_SCALE)
                    p = (e * (1.0 / jnp.sum(e, axis=-1, keepdims=True))).astype(BF)
                    oo = dot(p, v)
                    o_s[2 * j * n:2 * (j + 1) * n, t * 128:(t + 1) * 128] = jnp.where(low, oo[:2 * n], oo[2 * n:]).astype(BF)
            flush(len(pending))
            if c == 0:
                for cp in weights[l][1:]:
                    cp.wait()
            h = (load_rows(c) + dot(o_s[0:4 * n], wout[l])).astype(BF).astype(F32)
            normed = layer_norm(h, gains[2:3], gains[3:4])
            for m in range(0, HID, UP):
                hid_s[0:4 * n, m:m + UP] = gelu(dot(normed, wup[l, :, m:m + UP])).astype(BF)
            z = h + dot(hid_s[0:4 * n], wdown[l])
            for j in range(2):
                for b in range(2):
                    put(f_out, 2 * b + j, z[(2 * j + b) * n:(2 * j + b + 1) * n])
            zs = jnp.concatenate([f_out[t, 0:4 * n] for t in range(3)], axis=1).astype(BF)
            if l == BLOCKS - 1:
                zfin[start:start + n] = zs.reshape(n, 2, 2, D)
            else:
                zsend[l, start:start + n] = zs.reshape(n, 4, D)
            if l == 0 and c == 0:
                pl.semaphore_wait(barrier, DEV - 1)
            pending += [(l, c, k) for k in range(start, start + n)]
        flush(len(pending))
        if l < BLOCKS - 1:
            weights[l + 1][0].wait()
            lay_out(l + 1)

    for l in range(BLOCKS - 1):
        for c, (start, n) in enumerate(CHUNKS):
            sent = zsend.at[l, pl.ds(start, n - (start + n == DEV))]
            pltpu.make_async_copy(sent, sent, send_sem.at[l, c]).wait()
    pltpu.make_async_copy(zfin, y_ref, y_sem).wait()


def solution(mesh):
    table = [list(OFFS[start + r]) + [b] for start, n in CHUNKS for b in range(2) for r in range(n)]

    def local_stack(latents, norms, w_qkv, w_out, w_up, w_down):
        anywhere = pl.BlockSpec(memory_space=pl.ANY)
        dma = pltpu.SemaphoreType.DMA
        out = pl.pallas_call(
            stack_kernel,
            out_shape=jax.ShapeDtypeStruct((DEV, 2, 2, D), BF),
            in_specs=[anywhere] * 7,
            out_specs=anywhere,
            scratch_shapes=[
                pltpu.VMEM((2, SEQ, D), BF),
                pltpu.VMEM((SEQ, 5), jnp.int32),
                pltpu.VMEM((BLOCKS, 4, D), F32),
                pltpu.VMEM((BLOCKS, QKV, D), BF),
                pltpu.VMEM((BLOCKS, D, D), BF),
                pltpu.VMEM((BLOCKS, D, HID), BF),
                pltpu.VMEM((BLOCKS, HID, D), BF),
                pltpu.VMEM((D, QKV), BF),
                pltpu.VMEM((3, 2 * SEQ, 128), F32),
                pltpu.VMEM((3, 4 * BIG, 128), F32),
                pltpu.VMEM((2, SEQ, D), BF),
                pltpu.VMEM((2, SEQ, QKV), BF),
                pltpu.VMEM((4 * BIG, D), BF),
                pltpu.VMEM((4 * BIG, HID), BF),
                pltpu.VMEM((DEV, 2, 2, D), BF),
                pltpu.VMEM((BLOCKS - 1, DEV, 4, D), BF),
                pltpu.VMEM((BLOCKS - 1, DEV, 4, D), BF),
                dma((3,)),
                dma((BLOCKS, 4)),
                dma((BLOCKS - 1, len(CHUNKS))),
                dma((BLOCKS - 1, len(CHUNKS))),
                dma,
            ],
            compiler_params=pltpu.CompilerParams(collective_id=0, has_side_effects=True, vmem_limit_bytes=60 * 1024 * 1024),
            name='stack',
        )(latents.reshape(2, SEQ, D), jnp.asarray(table, jnp.int32), norms, jnp.transpose(w_qkv, (0, 2, 3, 4, 1)).reshape(BLOCKS, QKV, D),
          w_out.reshape(BLOCKS, D, D), w_up, w_down)
        return out.reshape(1, SEQ, 2, D)

    replicated = P()
    return jax.shard_map(local_stack, mesh=mesh, in_specs=(P('data', 'sp', None, None), replicated, replicated, replicated, replicated, replicated), out_specs=P('data', None, 'sp', None), check_vma=False)
```

```python
import math

import jax
import jax.numpy as jnp
from jax import lax
from jax.experimental import pallas as pl
from jax.experimental.pallas import tpu as pltpu
from jax.sharding import PartitionSpec as P

EPS = 1e-6
D = 384
QKV = 3 * D
HID = 4 * D
DEV = 128
SEQ = 2 * DEV
BLOCKS = 4
CUTS = (0, 64, 96, 128)
CHUNKS = tuple((a, b - a) for a, b in zip(CUTS, CUTS[1:]))
BIG = 64
UP = 512
HALVES = [[c for c, (start, n) in enumerate(CHUNKS) if start // 64 == half] for half in range(2)]
EXP_SCALE = 64 ** -0.5 * math.log2(math.e)
GELU_A = math.sqrt(2.0 / math.pi)
GELU_B = GELU_A * 0.044715
BF = jnp.bfloat16
F32 = jnp.float32


def slot_table():
    hops = (0, 1, 2, 1)
    offs = [(z, y, x, c) for z in range(4) for y in range(4) for x in range(4) for c in range(2)]

    def opposite(o):
        return (-o[0]) % 4, (-o[1]) % 4, (-o[2]) % 4, o[3]

    offs.sort(key=lambda o: (-(hops[o[0]] + hops[o[1]] + hops[o[2]]), -o[3], min(o, opposite(o)), o))
    index = {o: k for k, o in enumerate(offs)}
    back = [index[opposite(o)] for o in offs]
    assert all(start <= back[k] < start + n for start, n in CHUNKS for k in range(start, start + n))
    return offs, back


OFFS, BACK = slot_table()


def layer_norm(u, gain, shift):
    mean = jnp.mean(u, axis=-1, keepdims=True)
    cen = u - mean
    var = jnp.mean(cen * cen, axis=-1, keepdims=True)
    return (cen * lax.rsqrt(var + EPS) * gain + shift).astype(BF)


def gelu(x):
    half = 0.5 * x
    return half + half * jnp.tanh(x * (GELU_A + GELU_B * (x * x)))


def dot(a, b):
    return jnp.dot(a, b, preferred_element_type=F32)


def dot_t(a, b):
    return lax.dot_general(a, b, (((1,), (1,)), ((), ())), preferred_element_type=F32)


def put(ref, start, rows):
    n = rows.shape[0]
    for t in range(3):
        ref[t, pl.ds(start, n, stride=4), :] = rows[:, t * 128:(t + 1) * 128]


def take(ref, start, n):
    return jnp.concatenate([ref[t, pl.ds(start, n, stride=4), :] for t in range(3)], axis=1)


def stack_kernel(x_ref, tab_ref, norms_ref, wqkv_ref, wout_ref, wup_ref, wdown_ref, y_ref,
                 xv, tab, norms, wqkv, wout, wup, wdown, wq_s, f_in, f_out, a_s, qkv_s, o_s, hid_s, zfin, zsend, recv,
                 in_sem, w_sem, send_sem, recv_sem, y_sem):
    me = lax.axis_index('sp')
    digits = (me // 32, (me // 8) % 4, (me // 2) % 4, me % 2)
    barrier = pltpu.get_barrier_semaphore()

    def greet(i, carry):
        pl.semaphore_signal(barrier, inc=1, device_id={'sp': lax.rem(me + i, DEV)}, device_id_type=pl.DeviceIdType.MESH)
        return carry

    first = [pltpu.make_async_copy(src, dst, in_sem.at[i]) for i, (src, dst) in enumerate(((x_ref, xv), (tab_ref, tab), (norms_ref, norms)))]
    weights = [[pltpu.make_async_copy(src.at[l], dst.at[l], w_sem.at[l, i])
                for i, (src, dst) in enumerate(((wqkv_ref, wqkv), (wout_ref, wout), (wup_ref, wup), (wdown_ref, wdown)))]
               for l in range(BLOCKS)]
    for cp in first:
        cp.start()
    weights[0][0].start()
    lax.fori_loop(1, DEV, greet, 0)

    zpos = [(((digits[0] - d) + 4) % 4) * 32 for d in range(4)]
    ypos = [(((digits[1] - d) + 4) % 4) * 8 for d in range(4)]
    xpos = [(((digits[2] - d) + 4) % 4) * 2 for d in range(4)]
    cpos = [(digits[3] + d) % 2 for d in range(2)]

    def dev_of(k):
        o = OFFS[k]
        return zpos[o[0]] + ypos[o[1]] + xpos[o[2]] + cpos[o[3]]

    def send(l, c, k):
        if l == BLOCKS - 1:
            pltpu.make_async_copy(zfin.at[k], y_ref.at[dev_of(k)], y_sem).start()
        elif k < DEV - 1:
            pltpu.make_async_remote_copy(zsend.at[l, k], recv.at[l, BACK[k]], send_sem.at[l, c], recv_sem.at[l, c],
                                         device_id={'sp': dev_of(k)}, device_id_type=pl.DeviceIdType.MESH).start()

    def load_rows(c):
        start, n = CHUNKS[c]
        return jnp.concatenate([take(f_in, 4 * start + 2 * j + i, n) for j in range(2) for i in range(2)], axis=0)

    for cp in first:
        cp.wait()
    for cp in weights[0][1:]:
        cp.start()
    lane = lax.broadcasted_iota(jnp.int32, (SEQ, SEQ), 1)
    dz = (digits[0] - tab[:, 0:1] + 4) % 4
    dy = (digits[1] - tab[:, 1:2] + 4) % 4
    dx = (digits[2] - tab[:, 2:3] + 4) % 4
    dc = (digits[3] + tab[:, 3:4]) % 2
    patch = 2 * (dz * 32 + dy * 8 + dx * 2 + dc) + tab[:, 4:5]
    pick = jnp.where(lane == patch, 1.0, 0.0).astype(BF)
    for a in range(2):
        rows = dot(pick, xv[a])
        for start, n in CHUNKS:
            for b in range(2):
                put(f_in, 4 * start + 2 * a + b, rows[2 * start + b * n:2 * start + (b + 1) * n])

    pending = []

    def flush(count):
        for args in pending[:count]:
            send(*args)
        del pending[:count]

    def lay_out(l):
        for m in range(0, QKV, 384):
            wq_s[:, m:m + 384] = wqkv[l, m:m + 384].T

    weights[0][0].wait()
    lay_out(0)
    for l in range(BLOCKS):
        gains = norms[l]
        for c, (start, n) in enumerate(CHUNKS):
            if l > 0:
                last = start + n == DEV
                got = recv.at[l - 1, pl.ds(start, n - last)]
                pltpu.make_async_copy(got, got, recv_sem.at[l - 1, c]).wait()
                if last:
                    recv[l - 1, DEV - 1] = zsend[l - 1, DEV - 1]
                rows = recv[l - 1, start:start + n].reshape(4 * n, D).astype(F32)
                for t in range(3):
                    f_in[t, 4 * start:4 * (start + n), :] = rows[:, t * 128:(t + 1) * 128]
            normed = layer_norm(load_rows(c), gains[0:1], gains[1:2])
            for j in range(2):
                a_s[j, 2 * start:2 * (start + n), :] = normed[2 * j * n:2 * (j + 1) * n]
            if (start + n) % 64 == 0:
                r = 2 * (start + n) - 128
                normed = a_s[:, r:r + 128].reshape(256, D)
                for m in range(0, QKV, 384):
                    qkv_s[:, r:r + 128, m:m + 384] = dot(normed, wq_s[:, m:m + 384]).astype(BF).reshape(2, 128, 384)
        if l == 0:
            for row in weights[1:]:
                for cp in row:
                    cp.start()
        if l == BLOCKS - 1:
            plan = [(0, SEQ, (HALVES[0], HALVES[1]))]
        else:
            plan = [(0, 128, (HALVES[0],)), (128, 128, tuple((c,) for c in HALVES[1]))]
        for base, size, steps in plan:
            low = lax.broadcasted_iota(jnp.int32, (size, 128), 1) < 64
            flush(len(pending))
            for j in range(2):
                for t in range(3):
                    q = qkv_s[j, base:base + size, t * 128:(t + 1) * 128]
                    k = qkv_s[j, :, D + t * 128:D + (t + 1) * 128]
                    v = qkv_s[j, :, 2 * D + t * 128:2 * D + (t + 1) * 128]
                    zero = jnp.zeros_like(q)
                    s = dot_t(jnp.concatenate([jnp.where(low, q, zero), jnp.where(low, zero, q)], axis=0), k)
                    e = jnp.exp2((s - jnp.max(s, axis=-1, keepdims=True)) * EXP_SCALE)
                    p = (e * (1.0 / jnp.sum(e, axis=-1, keepdims=True))).astype(BF)
                    oo = dot(p, v)
                    o_s[j, base:base + size, t * 128:(t + 1) * 128] = jnp.where(low, oo[:size], oo[size:]).astype(BF)
            if base == 0:
                for cp in weights[l][1:]:
                    cp.wait()
            for step in steps:
                pieces = [CHUNKS[c] for c in step]
                total = sum(4 * n for _, n in pieces)
                mixed = jnp.concatenate([o_s[j, 2 * start:2 * (start + n), :] for start, n in pieces for j in range(2)], axis=0)
                h = (jnp.concatenate([load_rows(c) for c in step], axis=0) + dot(mixed, wout[l])).astype(BF).astype(F32)
                normed = layer_norm(h, gains[2:3], gains[3:4])
                flush(len(pending))
                for m in range(0, HID, UP):
                    hid_s[0:total, m:m + UP] = gelu(dot(normed, wup[l, :, m:m + UP])).astype(BF)
                z = h + dot(hid_s[0:total], wdown[l])
                row = 0
                for c in step:
                    start, n = CHUNKS[c]
                    for j in range(2):
                        for b in range(2):
                            put(f_out, 2 * b + j, z[row:row + n])
                            row += n
                    zs = jnp.concatenate([f_out[t, 0:4 * n] for t in range(3)], axis=1).astype(BF)
                    if l == BLOCKS - 1:
                        zfin[start:start + n] = zs.reshape(n, 2, 2, D)
                    else:
                        zsend[l, start:start + n] = zs.reshape(n, 4, D)
                    pending += [(l, c, k) for k in range(start, start + n)]
                if l == 0 and base == 0:
                    pl.semaphore_wait(barrier, DEV - 1)
        flush(len(pending))
        if l < BLOCKS - 1:
            weights[l + 1][0].wait()
            lay_out(l + 1)

    for l in range(BLOCKS - 1):
        for c, (start, n) in enumerate(CHUNKS):
            sent = zsend.at[l, pl.ds(start, n - (start + n == DEV))]
            pltpu.make_async_copy(sent, sent, send_sem.at[l, c]).wait()
    pltpu.make_async_copy(zfin, y_ref, y_sem).wait()


def solution(mesh):
    table = [list(OFFS[start + r]) + [b] for start, n in CHUNKS for b in range(2) for r in range(n)]

    def local_stack(latents, norms, w_qkv, w_out, w_up, w_down):
        anywhere = pl.BlockSpec(memory_space=pl.ANY)
        dma = pltpu.SemaphoreType.DMA
        out = pl.pallas_call(
            stack_kernel,
            out_shape=jax.ShapeDtypeStruct((DEV, 2, 2, D), BF),
            in_specs=[anywhere] * 7,
            out_specs=anywhere,
            scratch_shapes=[
                pltpu.VMEM((2, SEQ, D), BF),
                pltpu.VMEM((SEQ, 5), jnp.int32),
                pltpu.VMEM((BLOCKS, 4, D), F32),
                pltpu.VMEM((BLOCKS, QKV, D), BF),
                pltpu.VMEM((BLOCKS, D, D), BF),
                pltpu.VMEM((BLOCKS, D, HID), BF),
                pltpu.VMEM((BLOCKS, HID, D), BF),
                pltpu.VMEM((D, QKV), BF),
                pltpu.VMEM((3, 2 * SEQ, 128), F32),
                pltpu.VMEM((3, 4 * BIG, 128), F32),
                pltpu.VMEM((2, SEQ, D), BF),
                pltpu.VMEM((2, SEQ, QKV), BF),
                pltpu.VMEM((2, SEQ, D), BF),
                pltpu.VMEM((4 * BIG, HID), BF),
                pltpu.VMEM((DEV, 2, 2, D), BF),
                pltpu.VMEM((BLOCKS - 1, DEV, 4, D), BF),
                pltpu.VMEM((BLOCKS - 1, DEV, 4, D), BF),
                dma((3,)),
                dma((BLOCKS, 4)),
                dma((BLOCKS - 1, len(CHUNKS))),
                dma((BLOCKS - 1, len(CHUNKS))),
                dma,
            ],
            compiler_params=pltpu.CompilerParams(collective_id=0, has_side_effects=True, vmem_limit_bytes=60 * 1024 * 1024),
            name='stack',
        )(latents.reshape(2, SEQ, D), jnp.asarray(table, jnp.int32), norms, jnp.transpose(w_qkv, (0, 2, 3, 4, 1)).reshape(BLOCKS, QKV, D),
          w_out.reshape(BLOCKS, D, D), w_up, w_down)
        return out.reshape(1, SEQ, 2, D)

    replicated = P()
    return jax.shard_map(local_stack, mesh=mesh, in_specs=(P('data', 'sp', None, None), replicated, replicated, replicated, replicated, replicated), out_specs=P('data', None, 'sp', None), check_vma=False)
```

```python
import math

import jax
import jax.numpy as jnp
from jax import lax
from jax.experimental import pallas as pl
from jax.experimental.pallas import tpu as pltpu
from jax.sharding import PartitionSpec as P

EPS = 1e-6
D = 384
QKV = 3 * D
HID = 4 * D
DEV = 128
SEQ = 2 * DEV
BLOCKS = 4
CUTS = (0, 64, 96, 128)
CHUNKS = tuple((a, b - a) for a, b in zip(CUTS, CUTS[1:]))
BIG = 64
UP = 512
HALVES = [[c for c, (start, n) in enumerate(CHUNKS) if start // 64 == half] for half in range(2)]
EXP_SCALE = 64 ** -0.5 * math.log2(math.e)
GELU_A = math.sqrt(2.0 / math.pi)
GELU_B = GELU_A * 0.044715
BF = jnp.bfloat16
F32 = jnp.float32


def slot_table():
    hops = (0, 1, 2, 1)
    offs = [(z, y, x, c) for z in range(4) for y in range(4) for x in range(4) for c in range(2)]

    def opposite(o):
        return (-o[0]) % 4, (-o[1]) % 4, (-o[2]) % 4, o[3]

    offs.sort(key=lambda o: (-(hops[o[0]] + hops[o[1]] + hops[o[2]]), -o[3], min(o, opposite(o)), o))
    index = {o: k for k, o in enumerate(offs)}
    back = [index[opposite(o)] for o in offs]
    assert all(start <= back[k] < start + n for start, n in CHUNKS for k in range(start, start + n))
    return offs, back


OFFS, BACK = slot_table()


def layer_norm(u, gain, shift):
    mean = jnp.mean(u, axis=-1, keepdims=True)
    cen = u - mean
    var = jnp.mean(cen * cen, axis=-1, keepdims=True)
    return (cen * lax.rsqrt(var + EPS) * gain + shift).astype(BF)


def gelu(x):
    half = 0.5 * x
    return half + half * jnp.tanh(x * (GELU_A + GELU_B * (x * x)))


def dot(a, b):
    return jnp.dot(a, b, preferred_element_type=F32)


def dot_t(a, b):
    return lax.dot_general(a, b, (((1,), (1,)), ((), ())), preferred_element_type=F32)


def put(ref, start, rows):
    n = rows.shape[0]
    for t in range(3):
        ref[t, pl.ds(start, n, stride=4), :] = rows[:, t * 128:(t + 1) * 128]


def take(ref, start, n):
    return jnp.concatenate([ref[t, pl.ds(start, n, stride=4), :] for t in range(3)], axis=1)


def stack_kernel(x_ref, tab_ref, norms_ref, wqkv_ref, wout_ref, wup_ref, wdown_ref, y_ref,
                 xv, tab, norms, wqkv, wout, wup, wdown, wq_s, f_in, f_out, a_s, qkv_s, o_s, hid_s, zfin, zsend, recv,
                 in_sem, w_sem, send_sem, recv_sem, y_sem):
    me = lax.axis_index('sp')
    digits = (me // 32, (me // 8) % 4, (me // 2) % 4, me % 2)
    barrier = pltpu.get_barrier_semaphore()

    def greet(i, carry):
        pl.semaphore_signal(barrier, inc=1, device_id={'sp': lax.rem(me + i, DEV)}, device_id_type=pl.DeviceIdType.MESH)
        return carry

    first = [pltpu.make_async_copy(src, dst, in_sem.at[i]) for i, (src, dst) in enumerate(((x_ref, xv), (tab_ref, tab), (norms_ref, norms)))]
    weights = [[pltpu.make_async_copy(src.at[l], dst.at[l], w_sem.at[l, i])
                for i, (src, dst) in enumerate(((wqkv_ref, wqkv), (wout_ref, wout), (wup_ref, wup), (wdown_ref, wdown)))]
               for l in range(BLOCKS)]
    for cp in first:
        cp.start()
    weights[0][0].start()
    lax.fori_loop(1, DEV, greet, 0)

    zpos = [(((digits[0] - d) + 4) % 4) * 32 for d in range(4)]
    ypos = [(((digits[1] - d) + 4) % 4) * 8 for d in range(4)]
    xpos = [(((digits[2] - d) + 4) % 4) * 2 for d in range(4)]
    cpos = [(digits[3] + d) % 2 for d in range(2)]

    def dev_of(k):
        o = OFFS[k]
        return zpos[o[0]] + ypos[o[1]] + xpos[o[2]] + cpos[o[3]]

    def send(l, c, k):
        if l == BLOCKS - 1:
            pltpu.make_async_copy(zfin.at[k], y_ref.at[dev_of(k)], y_sem).start()
        elif k < DEV - 1:
            pltpu.make_async_remote_copy(zsend.at[l, k], recv.at[l, BACK[k]], send_sem.at[l, c], recv_sem.at[l, c],
                                         device_id={'sp': dev_of(k)}, device_id_type=pl.DeviceIdType.MESH).start()

    def load_rows(c):
        start, n = CHUNKS[c]
        return jnp.concatenate([take(f_in, 4 * start + 2 * j + i, n) for j in range(2) for i in range(2)], axis=0)

    for cp in first:
        cp.wait()
    for cp in weights[0][1:]:
        cp.start()
    lane = lax.broadcasted_iota(jnp.int32, (SEQ, SEQ), 1)
    dz = (digits[0] - tab[:, 0:1] + 4) % 4
    dy = (digits[1] - tab[:, 1:2] + 4) % 4
    dx = (digits[2] - tab[:, 2:3] + 4) % 4
    dc = (digits[3] + tab[:, 3:4]) % 2
    patch = 2 * (dz * 32 + dy * 8 + dx * 2 + dc) + tab[:, 4:5]
    pick = jnp.where(lane == patch, 1.0, 0.0).astype(BF)
    for a in range(2):
        rows = dot(pick, xv[a])
        for start, n in CHUNKS:
            for b in range(2):
                put(f_in, 4 * start + 2 * a + b, rows[2 * start + b * n:2 * start + (b + 1) * n])

    pending = []

    def flush(count):
        for args in pending[:count]:
            send(*args)
        del pending[:count]

    def lay_out(l):
        for m in range(0, QKV, 384):
            wq_s[:, m:m + 384] = wqkv[l, m:m + 384].T

    weights[0][0].wait()
    lay_out(0)
    for l in range(BLOCKS):
        gains = norms[l]
        for c, (start, n) in enumerate(CHUNKS):
            if l > 0:
                last = start + n == DEV
                got = recv.at[l - 1, pl.ds(start, n - last)]
                pltpu.make_async_copy(got, got, recv_sem.at[l - 1, c]).wait()
                if last:
                    recv[l - 1, DEV - 1] = zsend[l - 1, DEV - 1]
                rows = recv[l - 1, start:start + n].reshape(4 * n, D).astype(F32)
                for t in range(3):
                    f_in[t, 4 * start:4 * (start + n), :] = rows[:, t * 128:(t + 1) * 128]
            normed = layer_norm(load_rows(c), gains[0:1], gains[1:2])
            for j in range(2):
                a_s[j, 2 * start:2 * (start + n), :] = normed[2 * j * n:2 * (j + 1) * n]
            if (start + n) % 64 == 0:
                r = 2 * (start + n) - 128
                normed = a_s[:, r:r + 128].reshape(256, D)
                for m in range(0, QKV, 384):
                    qkv_s[:, r:r + 128, m:m + 384] = dot(normed, wq_s[:, m:m + 384]).astype(BF).reshape(2, 128, 384)
        if l == 0:
            for row in weights[1:]:
                for cp in row:
                    cp.start()
        if l == BLOCKS - 1:
            plan = [(0, SEQ, (HALVES[0], HALVES[1]))]
        else:
            plan = [(0, 128, (HALVES[0],)), (128, 128, tuple((c,) for c in HALVES[1]))]
        for base, size, steps in plan:
            low = lax.broadcasted_iota(jnp.int32, (size, 128), 1) < 64
            flush(len(pending))
            for j in range(2):
                for t in range(3):
                    q = qkv_s[j, base:base + size, t * 128:(t + 1) * 128]
                    k = qkv_s[j, :, D + t * 128:D + (t + 1) * 128]
                    v = qkv_s[j, :, 2 * D + t * 128:2 * D + (t + 1) * 128]
                    zero = jnp.zeros_like(q)
                    s = dot_t(jnp.concatenate([jnp.where(low, q, zero), jnp.where(low, zero, q)], axis=0), k)
                    e = jnp.exp2((s - jnp.max(s, axis=-1, keepdims=True)) * EXP_SCALE)
                    p = (e * (1.0 / jnp.sum(e, axis=-1, keepdims=True))).astype(BF)
                    oo = dot(p, v)
                    o_s[j, base:base + size, t * 128:(t + 1) * 128] = jnp.where(low, oo[:size], oo[size:]).astype(BF)
            if base == 0:
                for cp in weights[l][1:]:
                    cp.wait()
            for step in steps:
                flush(len(pending))
                pieces = [CHUNKS[c] for c in step]
                total = sum(4 * n for _, n in pieces)
                mixed = jnp.concatenate([o_s[j, 2 * start:2 * (start + n), :] for start, n in pieces for j in range(2)], axis=0)
                h = (jnp.concatenate([load_rows(c) for c in step], axis=0) + dot(mixed, wout[l])).astype(BF).astype(F32)
                normed = layer_norm(h, gains[2:3], gains[3:4])
                for m in range(0, HID, UP):
                    hid_s[0:total, m:m + UP] = gelu(dot(normed, wup[l, :, m:m + UP])).astype(BF)
                z = h + dot(hid_s[0:total], wdown[l])
                row = 0
                for c in step:
                    start, n = CHUNKS[c]
                    for j in range(2):
                        for b in range(2):
                            put(f_out, 2 * b + j, z[row:row + n])
                            row += n
                    zs = jnp.concatenate([f_out[t, 0:4 * n] for t in range(3)], axis=1).astype(BF)
                    if l == BLOCKS - 1:
                        zfin[start:start + n] = zs.reshape(n, 2, 2, D)
                    else:
                        zsend[l, start:start + n] = zs.reshape(n, 4, D)
                    pending += [(l, c, k) for k in range(start, start + n)]
                if l == 0 and base == 0:
                    pl.semaphore_wait(barrier, DEV - 1)
        flush(len(pending))
        if l < BLOCKS - 1:
            weights[l + 1][0].wait()
            lay_out(l + 1)

    for l in range(BLOCKS - 1):
        for c, (start, n) in enumerate(CHUNKS):
            sent = zsend.at[l, pl.ds(start, n - (start + n == DEV))]
            pltpu.make_async_copy(sent, sent, send_sem.at[l, c]).wait()
    pltpu.make_async_copy(zfin, y_ref, y_sem).wait()


def solution(mesh):
    table = [list(OFFS[start + r]) + [b] for start, n in CHUNKS for b in range(2) for r in range(n)]

    def local_stack(latents, norms, w_qkv, w_out, w_up, w_down):
        anywhere = pl.BlockSpec(memory_space=pl.ANY)
        dma = pltpu.SemaphoreType.DMA
        out = pl.pallas_call(
            stack_kernel,
            out_shape=jax.ShapeDtypeStruct((DEV, 2, 2, D), BF),
            in_specs=[anywhere] * 7,
            out_specs=anywhere,
            scratch_shapes=[
                pltpu.VMEM((2, SEQ, D), BF),
                pltpu.VMEM((SEQ, 5), jnp.int32),
                pltpu.VMEM((BLOCKS, 4, D), F32),
                pltpu.VMEM((BLOCKS, QKV, D), BF),
                pltpu.VMEM((BLOCKS, D, D), BF),
                pltpu.VMEM((BLOCKS, D, HID), BF),
                pltpu.VMEM((BLOCKS, HID, D), BF),
                pltpu.VMEM((D, QKV), BF),
                pltpu.VMEM((3, 2 * SEQ, 128), F32),
                pltpu.VMEM((3, 4 * BIG, 128), F32),
                pltpu.VMEM((2, SEQ, D), BF),
                pltpu.VMEM((2, SEQ, QKV), BF),
                pltpu.VMEM((2, SEQ, D), BF),
                pltpu.VMEM((4 * BIG, HID), BF),
                pltpu.VMEM((DEV, 2, 2, D), BF),
                pltpu.VMEM((BLOCKS - 1, DEV, 4, D), BF),
                pltpu.VMEM((BLOCKS - 1, DEV, 4, D), BF),
                dma((3,)),
                dma((BLOCKS, 4)),
                dma((BLOCKS - 1, len(CHUNKS))),
                dma((BLOCKS - 1, len(CHUNKS))),
                dma,
            ],
            compiler_params=pltpu.CompilerParams(collective_id=0, has_side_effects=True, vmem_limit_bytes=60 * 1024 * 1024),
            name='stack',
        )(latents.reshape(2, SEQ, D), jnp.asarray(table, jnp.int32), norms, jnp.transpose(w_qkv, (0, 2, 3, 4, 1)).reshape(BLOCKS, QKV, D),
          w_out.reshape(BLOCKS, D, D), w_up, w_down)
        return out.reshape(1, SEQ, 2, D)

    replicated = P()
    return jax.shard_map(local_stack, mesh=mesh, in_specs=(P('data', 'sp', None, None), replicated, replicated, replicated, replicated, replicated), out_specs=P('data', None, 'sp', None), check_vma=False)
```
